32 devices in a mesh: job: 2 (over y), aux: 16 (over z, x, core).
Axes of the slice: x: 2, y: 2, z: 4, core: 2. Of those that a mesh axis runs over, the one named last changes fastest.
Arguments:
- ints_ov: bfloat16 [256, 384, 384], P(('job', 'aux')), parts along dimension 0, may hold values from -0.3125 to 0.3125
- ints_oo: bfloat16 [256, 2, 384], P(('job', 'aux')), parts along dimension 0, may hold values from -1.5 to 1.5
- trial: bfloat16 [64, 4, 384], P('job'), parts along dimension 0, may hold values from -6 to 6
- occ_energy: float32 [64], P('job'), parts along dimension 0, may hold values from -1 to -0.2
- vir_energy: float32 [32000], P('job'), parts along dimension 0, may hold values from 0.2 to 2.5
- root_shift: float32 [8], P('job'), parts along dimension 0, may hold values from 0.1 to 0.6
- vir_blocks: int32 [32, 3], P('job'), parts along dimension 0, may hold values from 0 to 124, as said below
- pair_list: int32 [32, 4, 2], P('job'), parts along dimension 0, may hold values from 0 to 31, as said below
- pair_count: int32 [32], P('job'), parts along dimension 0, may hold values from 2 to 4, as said below
Outputs:
- sigma: float32 [64, 4, 384], P(('job', 'aux')), parts along dimension 0
The draws below stay inside these ranges and needn't reach their ends.
There are 2 independent parts, one for each index of `job`. The reference program is written for one: setup_inputs(seed, part) draws one part's arguments, and reference() takes and returns one part's arrays. A program takes and returns all parts, laid end to end along the dimension named above; each array names one. Nothing has to cross between parts.
Inputs may be any that keep to these rules, and one draw needn't show every extreme that they name: `pair_count`: some domain has 4 live pairs. `pair_list`: for domain d all 4 slots hold distinct pairs (i, j): i an occupied of domain d (d * 2 to d * 2 + 1) and j an occupied of one of the domains d + 1 to d + 3, taken cyclically modulo 16; slots from pair_count[d] on are not live. `vir_blocks`: the blocks of one domain are distinct.
All inputs are finite; a program needn't handle non-finite values.
Results may differ from the reference program's by a relative error of at most 0.00036.
Values may be sent and summed in bfloat16 or wider, within the bound.
A program may use at most 128 MiB of HBM per device.

```python
import math
import jax
import jax.numpy as jnp
from jax import lax

FB = 384
DV = 384
NV = 16000
K = 4
OD = 2
NN = 4
PMAX = 4
NDOM = 16
OCC = 32
SLAB = 8


def pair_tables(key):
    base_key = jax.random.fold_in(key, 7001)
    uniform_ints = jax.random.randint(jax.random.fold_in(base_key, 1), (NDOM,), 0, 16)
    counts = 2 + (uniform_ints >= 10).astype(jnp.int32) + (uniform_ints >= 14).astype(jnp.int32)
    counts = jnp.minimum(counts, PMAX)
    busiest = jax.random.randint(jax.random.fold_in(base_key, 2), (), 0, NDOM)
    domains = jnp.arange(NDOM, dtype=jnp.int32)
    counts = jnp.where(domains == busiest, PMAX, counts).astype(jnp.int32)
    options = OD * OD * (NN - 1)
    domain_keys = jax.random.split(jax.random.fold_in(base_key, 3), NDOM)
    chosen = jax.vmap(lambda one_key: jax.random.permutation(one_key, options)[:PMAX])(domain_keys).astype(jnp.int32)
    per_side = (NN - 1) * OD
    own_slot = chosen // per_side
    remainder = chosen % per_side
    ahead_by = 1 + remainder // OD
    other_slot = remainder % OD
    occ_first = domains[:, None] * OD + own_slot
    occ_second = (domains[:, None] + ahead_by) % NDOM * OD + other_slot
    return (counts, jnp.stack([occ_first, occ_second], axis=-1).astype(jnp.int32))


def draw_pair_list(key, part):
    return pair_tables(key)[1]


def draw_pair_count(key, part):
    return pair_tables(key)[0]


def draw_vir_blocks(key, part):
    domain_keys = jax.random.split(jax.random.fold_in(key, 9001), NDOM)
    chosen = jax.vmap(lambda one_key: jax.random.permutation(one_key, NV // 128)[:DV // 128])(domain_keys)
    return chosen.astype(jnp.int32)


def block_levels(own_key, shape, cuts, least, largest):
    gain, own = 1.0, jax.random.fold_in(own_key, 6)
    for axis_at, blocks in cuts:
        heights = jnp.exp(jax.random.uniform(jax.random.fold_in(own, axis_at), (blocks,), jnp.float32, least / len(cuts), largest / len(cuts)))
        gain = gain * jnp.repeat(heights, shape[axis_at] // blocks).reshape([-1 if axis == axis_at else 1 for axis in range(len(shape))])
    return gain


def noise(key, shape, width, most, shards=(), kind=jnp.bfloat16):
    factor_of = block_levels(key, shape, shards, -0.22, 0.18) if shards else 1.0
    array = jax.random.normal(key, shape, jnp.float32) * width * factor_of
    return jnp.minimum(jnp.maximum(array, -most), most).astype(kind)


def setup_inputs(seed: int = 0, part: int = 0) -> dict:
    arg_keys = jax.random.split(jax.random.key(seed), 10)
    own_keys = jax.random.split(jax.random.fold_in(arg_keys[9], part), 10)
    ints_ov = noise(own_keys[0], (NDOM * SLAB, FB, DV), FB ** -0.5, 0.3125, ((0, 16),))
    ints_oo = noise(own_keys[1], (NDOM * SLAB, OD, FB), 0.25, 1.5, ((0, 16),))
    trial = noise(own_keys[2], (OCC, K, DV), 1.0, 6.0)
    occ_energy = jnp.clip(jax.random.uniform(own_keys[3], (OCC,), jnp.float32, -1.0, -0.2), -1.0, -0.2)
    vir_energy = jnp.clip(jnp.exp(jax.random.uniform(own_keys[4], (NV,), jnp.float32, math.log(0.2), math.log(2.5))), 0.2, 2.5)
    root_shift = jnp.clip(jax.random.uniform(own_keys[5], (K,), jnp.float32, 0.1, 0.6), 0.1, 0.6)
    vir_blocks = draw_vir_blocks(jax.random.fold_in(jax.random.fold_in(arg_keys[9], part), 71), part)
    pair_list = draw_pair_list(jax.random.fold_in(jax.random.fold_in(arg_keys[9], part), 71), part)
    pair_count = draw_pair_count(jax.random.fold_in(jax.random.fold_in(arg_keys[9], part), 71), part)
    return dict(ints_ov=ints_ov, ints_oo=ints_oo, trial=trial, occ_energy=occ_energy, vir_energy=vir_energy, root_shift=root_shift, vir_blocks=vir_blocks, pair_list=pair_list, pair_count=pair_count)


def product(pattern, left_arg, right_arg):
    return jnp.einsum(pattern, left_arg.astype(jnp.float32), right_arg.astype(jnp.float32))


def reference(ints_ov, ints_oo, trial, occ_energy, vir_energy, root_shift, vir_blocks, pair_list, pair_count):
    slab_table = ints_ov.reshape(NDOM, SLAB, FB, DV)
    coupling_table = ints_oo.reshape(NDOM, SLAB, OD, FB)
    level_table = vir_energy.reshape(NV // 128, 128)

    def levels(domain):
        return jnp.take(level_table, vir_blocks[domain], axis=0).reshape(DV)

    def dressed(coupling, domain):
        occupied = lax.dynamic_slice_in_dim(trial, (domain * OD).astype(jnp.int32), OD, 0)
        return (-product("lq,lka->kqa", coupling, occupied)).astype(jnp.bfloat16)

    def deposit(accum_sigma, contribution, domain):
        start_row = (domain * OD).astype(jnp.int32)
        current = lax.dynamic_slice_in_dim(accum_sigma, start_row, OD, 0)
        return lax.dynamic_update_slice_in_dim(accum_sigma, current + contribution, start_row, 0)

    def visit(accum_sigma, flat_index):
        domain = flat_index // PMAX
        position = flat_index % PMAX
        occ_first = pair_list[domain, position, 0]
        occ_second = pair_list[domain, position, 1]
        partner = occ_second // OD
        row_first = occ_first - domain * OD
        row_second = ((partner - domain) % NDOM) * OD + occ_second % OD

        def pair_step(running):
            b_first = slab_table[domain, row_first]
            b_second = slab_table[domain, row_second]
            c_first = coupling_table[domain, row_first]
            c_second = coupling_table[domain, row_second]
            z_first = dressed(c_first, domain)
            z_second = dressed(c_second, partner)
            coupled = product("kqa,qb->kab", z_first, b_second) + product("qa,kqb->kab", b_first, z_second)
            denominator = levels(domain)[None, :, None] + levels(partner)[None, None, :] - occ_energy[occ_first] - occ_energy[occ_second] - root_shift[:, None, None]
            doubles = (coupled / denominator).astype(jnp.bfloat16)
            gamma_first = product("kab,qb->kqa", doubles, b_second).astype(jnp.bfloat16)
            gamma_second = product("kab,qa->kqb", doubles, b_first).astype(jnp.bfloat16)
            sigma_first = -product("lq,kqa->lka", c_first, gamma_first)
            sigma_second = -product("lq,kqb->lkb", c_second, gamma_second)
            running = deposit(running, sigma_first, domain)
            return deposit(running, sigma_second, partner)

        accum_sigma = lax.cond(pair_count[domain] > position, pair_step, lambda unchanged: unchanged, accum_sigma)
        return accum_sigma, None

    initial = jnp.zeros((OCC, K, DV), jnp.float32)
    accum_sigma, _ = lax.scan(visit, initial, jnp.arange(NDOM * PMAX, dtype=jnp.int32))
    return accum_sigma
```

```python
import functools

import jax
import jax.numpy as jnp
from jax import lax
from jax.experimental import pallas as pl
from jax.experimental.pallas import tpu as pltpu
from jax.sharding import PartitionSpec as P

F32 = jnp.float32
BF16 = jnp.bfloat16
LANES = 128


def split_high_low(value):
    high = value.astype(BF16).astype(F32)
    return high, (value - high).astype(BF16).astype(F32)


def sigma_kernel(
    ndomain, span, slot_count, occ_domain, root_count,
    ints_hbm, couple_hbm, trial_hbm, level_hbm, occ_energy, root_shift, pair_count, vir_blocks, pairs,
    out_ref,
    ints, couple, trial, level_table, levels_col, blocks_own, pairs_own, stage, landed,
    ints_sem, small_sem, send_sem, recv_sem,
):
    me = lax.axis_index("aux")
    slab_rows, fitting, virt = ints.shape
    width_blocks = virt // LANES
    rows = occ_domain * root_count

    def ahead(steps):
        return lax.rem(me + steps, ndomain)

    barrier = pltpu.get_barrier_semaphore()
    for steps in range(1, span):
        for other in (ahead(steps), ahead(ndomain - steps)):
            pl.semaphore_signal(
                barrier, inc=1, device_id={"aux": other}, device_id_type=pl.DeviceIdType.MESH
            )

    small = [
        pltpu.make_async_copy(pairs.at[me], pairs_own, small_sem.at[0]),
        pltpu.make_async_copy(couple_hbm, couple, small_sem.at[1]),
        pltpu.make_async_copy(level_hbm, level_table, small_sem.at[2]),
    ]
    for steps in range(span):
        small.append(
            pltpu.make_async_copy(
                vir_blocks.at[ahead(steps)], blocks_own.at[steps], small_sem.at[3 + 2 * steps]
            )
        )
        small.append(
            pltpu.make_async_copy(
                trial_hbm.at[pl.ds(ahead(steps) * occ_domain, occ_domain)],
                trial.at[pl.ds(steps * occ_domain, occ_domain)],
                small_sem.at[4 + 2 * steps],
            )
        )
    for copy in small:
        copy.start()
    big = [pltpu.make_async_copy(ints_hbm.at[row], ints.at[row], ints_sem.at[row]) for row in range(slab_rows)]
    for copy in big:
        copy.start()
    for copy in small:
        copy.wait()

    def level_rows(relative):
        return [level_table[pl.ds(blocks_own[relative, block], 1), :] for block in range(width_blocks)]

    for block, row in enumerate(level_rows(0)):
        levels_col[pl.ds(block * LANES, LANES), :] = jnp.broadcast_to(row, (LANES, LANES)).T

    row_index = lax.broadcasted_iota(jnp.int32, (rows, 1), 0)

    def trial_rows(relative):
        return jnp.concatenate(
            [trial[relative * occ_domain + own].astype(F32) for own in range(occ_domain)], axis=0
        )

    def couple_rows(slab_row):
        values = couple[slab_row].astype(F32)
        result = jnp.broadcast_to(values[0:1], (rows, fitting))
        for own in range(1, occ_domain):
            result = jnp.where(row_index >= own * root_count, values[own : own + 1], result)
        return result.astype(BF16)

    for copy in big:
        copy.wait()

    trial_first = trial_rows(0)
    live_slots = pair_count[me]

    def visit(slot, totals):
        occ_first = pairs_own[slot, 0]
        occ_second = pairs_own[slot, 1]
        relative = jnp.minimum(lax.rem(occ_second // occ_domain - me + ndomain, ndomain), span - 1)
        row_first = lax.rem(occ_first, occ_domain)
        row_second = relative * occ_domain + lax.rem(occ_second, occ_domain)

        mixed_first = jnp.dot(couple_rows(row_second), ints[row_first], preferred_element_type=F32)
        mixed_second = jnp.dot(couple_rows(row_first), ints[row_second], preferred_element_type=F32)
        first_high, first_low = split_high_low(mixed_first)
        second_high, second_low = split_high_low(mixed_second)
        trial_second = trial_rows(relative)
        left = jnp.concatenate([trial_first, trial_first, first_high, first_low], axis=0).T.astype(BF16)
        right = jnp.concatenate([second_high, second_low, trial_second, trial_second], axis=0)
        right_root = lax.broadcasted_iota(jnp.int32, (4 * rows, 1), 0) % root_count
        first_pair = jnp.concatenate([first_high, first_low], axis=0).astype(BF16)
        level_row = jnp.concatenate(level_rows(relative), axis=1) - occ_energy[occ_first] - occ_energy[occ_second]
        level_col = jnp.concatenate([levels_col[...]] * width_blocks, axis=1)

        sum_first = jnp.zeros((2 * rows, virt), F32)
        sum_second = jnp.zeros((rows, virt), F32)
        for root in range(root_count):
            right_now = jnp.where(right_root == root, right, 0.0).astype(BF16)
            coupled = jnp.dot(left, right_now, preferred_element_type=F32)
            doubles = (coupled / (level_col + (level_row - root_shift[root]))).astype(BF16)
            sum_first += lax.dot_general(
                right_now[: 2 * rows], doubles, (((1,), (1,)), ((), ())), preferred_element_type=F32
            )
            part = jnp.dot(first_pair, doubles, preferred_element_type=F32)
            part = part[:rows] + part[rows:]
            sum_second += jnp.where(row_index % root_count == root, part, 0.0)
        live = live_slots > slot
        sum_first = jnp.where(live, sum_first[:rows] + sum_first[rows:], 0.0)
        new_totals = [totals[0] + sum_first]
        for steps in range(1, span):
            new_totals.append(
                totals[steps] + jnp.where(jnp.logical_and(live, relative == steps), sum_second, 0.0)
            )
        return tuple(new_totals)

    totals = tuple(jnp.zeros((rows, virt), F32) for _ in range(span))
    if UNROLL:
        for slot in range(slot_count):
            totals = visit(slot, totals)
    else:
        totals = lax.fori_loop(0, slot_count, visit, totals)

    for steps in range(1, span):
        stage[steps - 1] = totals[steps]
    pl.semaphore_wait(barrier, 2 * (span - 1))
    copies = []
    for steps in range(1, span):
        copy = pltpu.make_async_remote_copy(
            src_ref=stage.at[steps - 1],
            dst_ref=landed.at[steps - 1],
            send_sem=send_sem.at[steps - 1],
            recv_sem=recv_sem.at[steps - 1],
            device_id={"aux": ahead(steps)},
            device_id_type=pl.DeviceIdType.MESH,
        )
        copy.start()
        copies.append(copy)
    result = totals[0]
    for copy in copies:
        copy.wait()
    for steps in range(1, span):
        result = result + landed[steps - 1]
    for own in range(occ_domain):
        out_ref[own] = result[own * root_count : (own + 1) * root_count]


UNROLL = True


def per_device(
    ints_ov, ints_oo, trial, occ_energy, vir_energy, root_shift, vir_blocks, pair_list, pair_count
):
    slab_rows, fitting, virt = ints_ov.shape
    occ_domain = ints_oo.shape[1]
    root_count = trial.shape[1]
    slot_count = pair_list.shape[1]
    span = slab_rows // occ_domain
    rows = occ_domain * root_count
    level_table = vir_energy.reshape(-1, LANES)
    anywhere = pl.BlockSpec(memory_space=pl.ANY)
    scalars = pl.BlockSpec(memory_space=pltpu.SMEM)
    return pl.pallas_call(
        functools.partial(
            sigma_kernel, lax.axis_size("aux"), span, slot_count, occ_domain, root_count
        ),
        out_shape=jax.ShapeDtypeStruct((occ_domain, root_count, virt), F32),
        in_specs=[anywhere] * 4 + [scalars] * 3 + [anywhere] * 2,
        out_specs=pl.BlockSpec(memory_space=pltpu.VMEM),
        scratch_shapes=[
            pltpu.VMEM(ints_ov.shape, BF16),
            pltpu.VMEM(ints_oo.shape, BF16),
            pltpu.VMEM((span * occ_domain, root_count, virt), BF16),
            pltpu.VMEM(level_table.shape, F32),
            pltpu.VMEM((virt, LANES), F32),
            pltpu.SMEM((span, vir_blocks.shape[1]), jnp.int32),
            pltpu.SMEM(pair_list.shape[1:], jnp.int32),
            pltpu.VMEM((span - 1, rows, virt), F32),
            pltpu.VMEM((span - 1, rows, virt), F32),
            pltpu.SemaphoreType.DMA((slab_rows,)),
            pltpu.SemaphoreType.DMA((3 + 2 * span,)),
            pltpu.SemaphoreType.DMA((span - 1,)),
            pltpu.SemaphoreType.DMA((span - 1,)),
        ],
        compiler_params=pltpu.CompilerParams(collective_id=0, has_side_effects=True),
        name="sigma",
    )(
        ints_ov, ints_oo, trial, level_table, occ_energy, root_shift, pair_count, vir_blocks, pair_list
    )


def solution(mesh):
    in_specs = (
        P(("job", "aux"), None, None),
        P(("job", "aux"), None, None),
        P("job", None, None),
        P("job"),
        P("job"),
        P("job"),
        P("job", None),
        P("job", None, None),
        P("job"),
    )
    out_specs = P(("job", "aux"), None, None)
    return jax.shard_map(
        per_device, mesh=mesh, in_specs=in_specs, out_specs=out_specs, check_vma=False
    )
```

```python
import functools

import jax
import jax.numpy as jnp
from jax import lax
from jax.experimental import pallas as pl
from jax.experimental.pallas import tpu as pltpu
from jax.sharding import PartitionSpec as P

F32 = jnp.float32
BF16 = jnp.bfloat16
LANES = 128


def split_high_low(value):
    high = value.astype(BF16).astype(F32)
    return high, (value - high).astype(BF16).astype(F32)


def sigma_kernel(
    ndomain, span, slot_count, occ_domain, root_count,
    ints_hbm, couple_hbm, trial_hbm, level_hbm, occ_energy, root_shift, pair_count, vir_blocks, pairs,
    out_ref,
    ints, couple, trial, level_table, levels_col, mixed_own, mixed_far, doubles, stage, landed,
    ints_sem, small_sem, send_sem, recv_sem,
):
    me = lax.axis_index("aux")
    slab_rows, fitting, virt = ints.shape
    width_blocks = virt // LANES
    rows = occ_domain * root_count

    def ahead(steps):
        return lax.rem(me + steps, ndomain)

    barrier = pltpu.get_barrier_semaphore()
    for steps in range(1, span):
        for other in (ahead(steps), ahead(ndomain - steps)):
            pl.semaphore_signal(
                barrier, inc=1, device_id={"aux": other}, device_id_type=pl.DeviceIdType.MESH
            )

    small = [
        pltpu.make_async_copy(couple_hbm, couple, small_sem.at[0]),
        pltpu.make_async_copy(level_hbm, level_table, small_sem.at[1]),
    ]
    for steps in range(span):
        small.append(
            pltpu.make_async_copy(
                trial_hbm.at[pl.ds(ahead(steps) * occ_domain, occ_domain)],
                trial.at[pl.ds(steps * occ_domain, occ_domain)],
                small_sem.at[2 + steps],
            )
        )
    for copy in small:
        copy.start()
    big = [pltpu.make_async_copy(ints_hbm.at[row], ints.at[row], ints_sem.at[row]) for row in range(slab_rows)]
    for copy in big:
        copy.start()
    for copy in small:
        copy.wait()

    def level_rows(relative):
        return [level_table[pl.ds(vir_blocks[block, ahead(relative)], 1), :] for block in range(width_blocks)]

    for block, row in enumerate(level_rows(0)):
        levels_col[pl.ds(block * LANES, LANES), :] = jnp.broadcast_to(row, (LANES, LANES)).T

    row_index = lax.broadcasted_iota(jnp.int32, (rows, 1), 0)

    def trial_rows(relative):
        return jnp.concatenate(
            [trial[relative * occ_domain + own].astype(F32) for own in range(occ_domain)], axis=0
        )

    def couple_rows(slab_row):
        values = couple[slab_row].astype(F32)
        result = jnp.broadcast_to(values[0:1], (rows, fitting))
        for own in range(1, occ_domain):
            result = jnp.where(row_index >= own * root_count, values[own : own + 1], result)
        return result.astype(BF16)

    couple_all = [couple_rows(row) for row in range(slab_rows)]
    own_couple = jnp.concatenate(couple_all[:occ_domain], axis=0)
    far_couple = jnp.concatenate(couple_all[occ_domain:], axis=0)
    far_rows = slab_rows - occ_domain
    for row in range(slab_rows):
        big[row].wait()
        if row < occ_domain:
            mixed = jnp.dot(far_couple, ints[row], preferred_element_type=F32)
            for far in range(far_rows):
                mixed_own[row * far_rows + far] = mixed[far * rows : (far + 1) * rows]
        else:
            mixed = jnp.dot(own_couple, ints[row], preferred_element_type=F32)
            for own in range(occ_domain):
                mixed_far[own * far_rows + row - occ_domain] = mixed[own * rows : (own + 1) * rows]

    trial_first = trial_rows(0)
    live_slots = pair_count[me]
    right_root = lax.broadcasted_iota(jnp.int32, (4 * rows, 1), 0) % root_count
    totals = [jnp.zeros((rows, virt), F32) for _ in range(span)]
    weights = []
    for slot in range(slot_count):
        occ_first = pairs[slot, 0, me]
        occ_second = pairs[slot, 1, me]
        relative = lax.rem(occ_second // occ_domain - me + ndomain, ndomain)
        relative = jnp.maximum(jnp.minimum(relative, span - 1), 1)
        own = lax.rem(occ_first, occ_domain)
        place = own * far_rows + (relative - 1) * occ_domain + lax.rem(occ_second, occ_domain)
        live = live_slots > slot

        first_high, first_low = split_high_low(mixed_own[place])
        second_high, second_low = split_high_low(mixed_far[place])
        trial_second = trial_rows(relative)
        left = jnp.concatenate([trial_first, trial_first, first_high, first_low], axis=0).T.astype(BF16)
        right = jnp.concatenate([second_high, second_low, trial_second, trial_second], axis=0)
        right = jnp.concatenate(
            [jnp.where(right_root == root, right, 0.0) for root in range(root_count)], axis=1
        ).astype(BF16)
        first_pair = jnp.concatenate([first_high, first_low], axis=0).astype(BF16)
        level_row = jnp.concatenate(level_rows(relative), axis=1) - occ_energy[occ_first] - occ_energy[occ_second]
        level_row = jnp.concatenate([level_row - root_shift[root] for root in range(root_count)], axis=1)
        level_col = jnp.concatenate([levels_col[...]] * (width_blocks * root_count), axis=1)

        coupled = jnp.dot(left, right, preferred_element_type=F32)
        answer = (coupled / (level_col + level_row)).astype(BF16)
        doubles[slot] = answer
        weights.append(right[: 2 * rows])
        part = jnp.dot(first_pair, answer, preferred_element_type=F32)
        part = part[:rows] + part[rows:]
        second = jnp.zeros((rows, virt), F32)
        for root in range(root_count):
            second += jnp.where(
                row_index % root_count == root, part[:, root * virt : (root + 1) * virt], 0.0
            )
        for steps in range(1, span):
            totals[steps] += jnp.where(jnp.logical_and(live, relative == steps), second, 0.0)

    for steps in range(1, span):
        stage[steps - 1] = totals[steps]
    pl.semaphore_wait(barrier, 2 * (span - 1))
    copies = []
    for steps in range(1, span):
        copy = pltpu.make_async_remote_copy(
            src_ref=stage.at[steps - 1],
            dst_ref=landed.at[steps - 1],
            send_sem=send_sem.at[steps - 1],
            recv_sem=recv_sem.at[steps - 1],
            device_id={"aux": ahead(steps)},
            device_id_type=pl.DeviceIdType.MESH,
        )
        copy.start()
        copies.append(copy)
    result = totals[0]
    for slot in range(slot_count):
        first = lax.dot_general(
            weights[slot], doubles[slot], (((1,), (1,)), ((), ())), preferred_element_type=F32
        )
        result += jnp.where(live_slots > slot, first[:rows] + first[rows:], 0.0)
    for copy in copies:
        copy.wait()
    for steps in range(1, span):
        result = result + landed[steps - 1]
    for own in range(occ_domain):
        out_ref[own] = result[own * root_count : (own + 1) * root_count]


def per_device(
    ints_ov, ints_oo, trial, occ_energy, vir_energy, root_shift, vir_blocks, pair_list, pair_count
):
    slab_rows, fitting, virt = ints_ov.shape
    occ_domain = ints_oo.shape[1]
    root_count = trial.shape[1]
    slot_count = pair_list.shape[1]
    span = slab_rows // occ_domain
    rows = occ_domain * root_count
    level_table = vir_energy.reshape(-1, LANES)
    anywhere = pl.BlockSpec(memory_space=pl.ANY)
    scalars = pl.BlockSpec(memory_space=pltpu.SMEM)
    return pl.pallas_call(
        functools.partial(
            sigma_kernel, lax.axis_size("aux"), span, slot_count, occ_domain, root_count
        ),
        out_shape=jax.ShapeDtypeStruct((occ_domain, root_count, virt), F32),
        in_specs=[anywhere] * 4 + [scalars] * 5,
        out_specs=pl.BlockSpec(memory_space=pltpu.VMEM),
        scratch_shapes=[
            pltpu.VMEM(ints_ov.shape, BF16),
            pltpu.VMEM(ints_oo.shape, BF16),
            pltpu.VMEM((span * occ_domain, root_count, virt), BF16),
            pltpu.VMEM(level_table.shape, F32),
            pltpu.VMEM((virt, LANES), F32),
            pltpu.VMEM((occ_domain * (slab_rows - occ_domain), rows, virt), F32),
            pltpu.VMEM((occ_domain * (slab_rows - occ_domain), rows, virt), F32),
            pltpu.VMEM((slot_count, virt, root_count * virt), BF16),
            pltpu.VMEM((span - 1, rows, virt), F32),
            pltpu.VMEM((span - 1, rows, virt), F32),
            pltpu.SemaphoreType.DMA((slab_rows,)),
            pltpu.SemaphoreType.DMA((2 + span,)),
            pltpu.SemaphoreType.DMA((span - 1,)),
            pltpu.SemaphoreType.DMA((span - 1,)),
        ],
        compiler_params=pltpu.CompilerParams(collective_id=0, has_side_effects=True),
        name="sigma",
    )(
        ints_ov, ints_oo, trial, level_table, occ_energy, root_shift, pair_count, vir_blocks.T,
        pair_list.transpose(1, 2, 0),
    )


def solution(mesh):
    in_specs = (
        P(("job", "aux"), None, None),
        P(("job", "aux"), None, None),
        P("job", None, None),
        P("job"),
        P("job"),
        P("job"),
        P("job", None),
        P("job", None, None),
        P("job"),
    )
    out_specs = P(("job", "aux"), None, None)
    return jax.shard_map(
        per_device, mesh=mesh, in_specs=in_specs, out_specs=out_specs, check_vma=False
    )
```
